32 devices in a mesh: tm: 4 (over y, x), slab: 8 (over z, core).
Axes of the slice: x: 2, y: 2, z: 4, core: 2. Of those that a mesh axis runs over, the one named last changes fastest.
Arguments:
- velocity: bfloat16 [4, 3, 2, 131072], P('tm', None, None, 'slab'), may hold values from -64 to 64
- shell_index: int32 [131072], P('slab'), may hold values from 0 to 127, as said below
- ref_order: int32 [4], replicated, may hold values from 0 to 3, each once
Outputs:
- coherence: float32 [4, 4, 128], P('tm')
- spectrum: float32 [4, 128], P('tm')
The draws below stay inside these ranges and needn't reach their ends.
Inputs may be any that keep to these rules, and one draw needn't show every extreme that they name: `shell_index`: every shell number from 0 to 127 is taken by some mode. `ref_order`: each snapshot number appears once.
All inputs are finite; a program needn't handle non-finite values.
Results may differ from the reference program's by a relative error of at most 0.0003.
Values may be sent and summed in bfloat16 or wider, within the bound.
A program may use at most 64 MiB of HBM per device.

```python
import math
import jax
import jax.numpy as jnp
from jax import lax

SHELLS = 128
SNAPS = 4
MODES = 131072


def draw_velocity(key, part):
    keys = jax.random.split(jax.random.fold_in(key, 11), 5)
    amplitude = jnp.exp(jax.random.uniform(keys[0], (MODES,), jnp.float32, 0.0, math.log(10.0)))
    noise = jnp.clip(jax.random.normal(keys[1], (SNAPS, 3, 2, MODES), jnp.float32), -4.0, 4.0)
    persist = jax.random.uniform(keys[2], (MODES,), jnp.float32, 0.3, 0.97)
    scaling = jnp.exp(jax.random.uniform(keys[3], (SNAPS, 64), jnp.float32, math.log(0.5), math.log(2.0)))
    turning = jax.random.uniform(keys[4], (MODES,), jnp.float32, 0.2, 1.0)
    keep_share = jnp.sqrt(1.0 - persist * persist)

    def advance(state, fresh):
        new_state = persist * state + keep_share * fresh
        return (new_state, new_state)
    last_state, states = lax.scan(advance, noise[0], noise[1:])
    states = jnp.concatenate([noise[0][None], states], axis=0)
    steps_taken = jnp.arange(SNAPS, dtype=jnp.int32).astype(jnp.float32)
    phase = steps_taken[:, None] * turning[None, :]
    cosine = jnp.cos(phase)[:, None, :]
    sine = jnp.sin(phase)[:, None, :]
    real_old = states[:, :, 0]
    imag_old = states[:, :, 1]
    real_new = real_old * cosine - imag_old * sine
    imag_new = real_old * sine + imag_old * cosine
    states = jnp.stack([real_new, imag_new], axis=2)
    position = jnp.arange(MODES, dtype=jnp.int32)
    band = position * 64 // MODES
    band_scale = scaling[:, band]
    values = states * amplitude[None, None, None, :] * band_scale[:, None, None, :]
    return jnp.clip(values, -64.0, 64.0).astype(jnp.bfloat16)


def draw_shell_index(key, part):
    first_draw = jax.random.randint(jax.random.fold_in(key, 23), (MODES,), 0, SHELLS, dtype=jnp.int32)
    second_draw = jax.random.randint(jax.random.fold_in(key, 29), (MODES,), 0, SHELLS, dtype=jnp.int32)
    drawn = jnp.maximum(first_draw, second_draw)
    position = jnp.arange(MODES, dtype=jnp.int32)
    stride = MODES // SHELLS
    forced = position // stride % SHELLS
    return jnp.where(position % stride == 0, forced, drawn).astype(jnp.int32)


def setup_inputs(seed: int = 0) -> dict:
    streams_of = jax.random.split(jax.random.key(seed), 4)
    velocity = draw_velocity(jax.random.fold_in(streams_of[3], 71), 0)
    shell_index = draw_shell_index(jax.random.fold_in(streams_of[3], 71), 0)
    ref_order = jax.random.permutation(streams_of[2], SNAPS).astype(jnp.int32)
    return dict(velocity=velocity, shell_index=shell_index, ref_order=ref_order)


def reference(velocity, shell_index, ref_order):
    fields = velocity.astype(jnp.float32)
    rotated = jnp.stack([fields[:, :, 1], -fields[:, :, 0]], axis=2)
    energy = jnp.sum(fields * fields, axis=(1, 2)).astype(jnp.bfloat16)
    energy = lax.optimization_barrier(energy).astype(jnp.float32)
    spectrum = jax.ops.segment_sum(energy.T, shell_index, num_segments=SHELLS).T

    def one_snapshot(snapshot):
        own_field = lax.dynamic_index_in_dim(fields, snapshot, 0, keepdims=False)
        own_rotated = lax.dynamic_index_in_dim(rotated, snapshot, 0, keepdims=False)
        real_part = jnp.einsum("cpm,scpm->sm", own_field, fields, precision=lax.Precision.HIGHEST)
        imag_part = jnp.einsum("cpm,scpm->sm", own_rotated, fields, precision=lax.Precision.HIGHEST)
        stacked = jnp.stack([real_part, imag_part], axis=0).astype(jnp.bfloat16)
        stacked = lax.optimization_barrier(stacked).astype(jnp.float32)
        binned = jax.ops.segment_sum(stacked.reshape(2 * SNAPS, MODES).T, shell_index, num_segments=SHELLS)
        return binned.T.reshape(2, SNAPS, SHELLS)

    pair_sums = lax.map(one_snapshot, jnp.arange(SNAPS, dtype=jnp.int32))
    chosen = pair_sums[:, :, ref_order]
    power_sum = chosen[:, 0] * chosen[:, 0] + chosen[:, 1] * chosen[:, 1]
    coherence = power_sum / (spectrum[:, None, :] * spectrum[ref_order][None, :, :])
    return coherence, spectrum
```

```python
import functools

import jax
import jax.numpy as jnp
from jax import lax
from jax.experimental import pallas as pl
from jax.experimental.pallas import tpu as pltpu
from jax.sharding import PartitionSpec as P

SHELLS = 128
LANES = 128
CORES = 2
MESH = pl.DeviceIdType.MESH


def kernel(
    snaps, slabs, rows,
    vel_ref, ids_ref, order_ref,
    coh_ref, spec_ref,
    staged, ids, got, split, terms, lhs, hot, mine, near, mid, far, total, ready,
    load_sem, send_sem, recv_sem, near_send, near_recv, far_send, far_recv,
):
    tm = lax.axis_index("tm")
    slab = lax.axis_index("slab")
    core = lax.rem(slab, CORES)
    place = lax.div(slab, CORES)
    places = slabs // CORES
    pairs = snaps * snaps

    load_vel = pltpu.make_async_copy(vel_ref, staged, load_sem.at[0])
    load_vel.start()
    load_ids = pltpu.make_async_copy(
        ids_ref.at[pl.ds(pl.multiple_of(tm * rows, rows), rows)], ids, load_sem.at[1]
    )
    load_ids.start()
    own = pl.ds(pl.multiple_of(tm * 2 * rows, 2 * rows), 2 * rows)
    load_own = pltpu.make_async_copy(vel_ref.at[:, own], got.at[tm], load_sem.at[2])
    load_own.start()

    near_peers = []
    for offset in range(1, snaps * CORES):
        other = lax.rem(tm + offset // CORES, snaps)
        other_core = lax.rem(core + offset % CORES, CORES)
        near_peers.append((other, place * CORES + other_core))
    far_peers = []
    for offset in range(1, places):
        far_peers.append((tm, lax.rem(place + offset, places) * CORES + core))

    barrier = pltpu.get_barrier_semaphore()
    for peer in near_peers + far_peers:
        pl.semaphore_signal(barrier, inc=1, device_id=peer, device_id_type=MESH)

    load_ids.wait()
    shell = lax.broadcasted_iota(jnp.int32, (SHELLS, LANES), 0)
    for j in range(rows):
        same = shell == jnp.broadcast_to(ids[j : j + 1, :], (SHELLS, LANES))
        hot[:, j * LANES : (j + 1) * LANES] = jnp.where(same, 1.0, 0.0).astype(jnp.bfloat16)

    load_vel.wait()
    pl.semaphore_wait(barrier, len(near_peers) + len(far_peers))

    moves = []
    for offset in range(1, snaps):
        other = lax.rem(tm + offset, snaps)
        share = pl.ds(pl.multiple_of(other * 2 * rows, 2 * rows), 2 * rows)
        move = pltpu.make_async_remote_copy(
            src_ref=staged.at[:, share],
            dst_ref=got.at[tm],
            send_sem=send_sem.at[offset],
            recv_sem=recv_sem.at[offset],
            device_id=(other, slab),
            device_id_type=MESH,
        )
        move.start()
        moves.append(move)
    load_own.wait()
    for move in moves:
        move.wait()

    real, imag = {}, {}
    for t in range(snaps):
        for c in range(3):
            split[t * 3 + c] = got[t, c].astype(jnp.float32)
    for t in range(snaps):
        for c in range(3):
            real[t, c] = split[t * 3 + c, pl.ds(0, rows, stride=2), :]
            imag[t, c] = split[t * 3 + c, pl.ds(1, rows, stride=2), :]

    for t in range(snaps):
        for r in range(t, snaps):
            value = real[t, 0] * real[r, 0] + imag[t, 0] * imag[r, 0]
            for c in (1, 2):
                value = value + real[t, c] * real[r, c]
                value = value + imag[t, c] * imag[r, c]
            terms[(t * snaps + r) * rows : (t * snaps + r + 1) * rows] = value
            if r > t:
                value = imag[t, 0] * real[r, 0] - real[t, 0] * imag[r, 0]
                for c in (1, 2):
                    value = value + imag[t, c] * real[r, c]
                    value = value - real[t, c] * imag[r, c]
                terms[(r * snaps + t) * rows : (r * snaps + t + 1) * rows] = value
    for j in range(rows):
        block = terms[pl.ds(j, pairs, stride=rows), :]
        lhs[:, j * LANES : (j + 1) * LANES] = block.astype(jnp.bfloat16)
    mine[...] = lax.dot_general(
        lhs[...], hot[...], (((1,), (1,)), ((), ())), preferred_element_type=jnp.float32
    )

    def spread(source, slots, slot_of_me, peers, send, recv):
        copies = []
        for n, peer in enumerate(peers):
            copy = pltpu.make_async_remote_copy(
                src_ref=source,
                dst_ref=slots.at[n],
                send_sem=send.at[n],
                recv_sem=recv.at[n],
                device_id=peer,
                device_id_type=MESH,
            )
            copy.start()
            copies.append(copy)
        for copy in copies:
            copy.wait()
        value = source[...]
        for n in range(len(peers)):
            value = value + slots[n]
        return value

    mid[...] = spread(mine, near, None, near_peers, near_send, near_recv)
    total[...] = spread(mid, far, None, far_peers, far_send, far_recv)

    spectra = total[pl.ds(0, snaps, stride=snaps + 1), :]
    own_spectrum = total[pl.ds(tm * (snaps + 1), 1), :]
    across = total[pl.ds(tm * snaps, snaps), :]
    down = total[pl.ds(tm, snaps, stride=snaps), :]
    which = lax.broadcasted_iota(jnp.int32, (snaps, SHELLS), 0)
    down = jnp.where(which == tm, 0.0, down)
    ready[...] = (across * across + down * down) / (own_spectrum * spectra)
    for j in range(snaps):
        coh_ref[0, j : j + 1, :] = ready[pl.ds(order_ref[j], 1), :]
    spec_ref[...] = own_spectrum


def body(velocity, shell_index, ref_order):
    snaps = lax.axis_size("tm")
    slabs = lax.axis_size("slab")
    modes = velocity.shape[3]
    blocks = modes // LANES
    rows = blocks // snaps
    pairs = snaps * snaps
    vel = velocity.reshape(3, 2, blocks, LANES).transpose(0, 2, 1, 3)
    vel = vel.reshape(3, 2 * blocks, LANES)
    ids = shell_index.reshape(blocks, LANES)
    near = snaps * CORES - 1
    far = slabs // CORES - 1
    return pl.pallas_call(
        functools.partial(kernel, snaps, slabs, rows),
        out_shape=(
            jax.ShapeDtypeStruct((1, snaps, SHELLS), jnp.float32),
            jax.ShapeDtypeStruct((1, SHELLS), jnp.float32),
        ),
        in_specs=[
            pl.BlockSpec(memory_space=pl.ANY),
            pl.BlockSpec(memory_space=pl.ANY),
            pl.BlockSpec(memory_space=pltpu.SMEM),
        ],
        out_specs=(
            pl.BlockSpec(memory_space=pltpu.VMEM),
            pl.BlockSpec(memory_space=pltpu.VMEM),
        ),
        scratch_shapes=[
            pltpu.VMEM((3, 2 * blocks, LANES), jnp.bfloat16),
            pltpu.VMEM((rows, LANES), jnp.int32),
            pltpu.VMEM((snaps, 3, 2 * rows, LANES), jnp.bfloat16),
            pltpu.VMEM((snaps * 3, 2 * rows, LANES), jnp.float32),
            pltpu.VMEM((pairs * rows, LANES), jnp.float32),
            pltpu.VMEM((pairs, rows * LANES), jnp.bfloat16),
            pltpu.VMEM((SHELLS, rows * LANES), jnp.bfloat16),
            pltpu.VMEM((pairs, SHELLS), jnp.float32),
            pltpu.VMEM((near, pairs, SHELLS), jnp.float32),
            pltpu.VMEM((pairs, SHELLS), jnp.float32),
            pltpu.VMEM((far, pairs, SHELLS), jnp.float32),
            pltpu.VMEM((pairs, SHELLS), jnp.float32),
            pltpu.VMEM((snaps, SHELLS), jnp.float32),
            pltpu.SemaphoreType.DMA((3,)),
            pltpu.SemaphoreType.DMA((snaps,)),
            pltpu.SemaphoreType.DMA((snaps,)),
            pltpu.SemaphoreType.DMA((near,)),
            pltpu.SemaphoreType.DMA((near,)),
            pltpu.SemaphoreType.DMA((far,)),
            pltpu.SemaphoreType.DMA((far,)),
        ],
        compiler_params=pltpu.CompilerParams(collective_id=0, has_side_effects=True),
    )(vel, ids, ref_order)


def solution(mesh):
    in_specs = (P("tm", None, None, "slab"), P("slab"), P())
    out_specs = (P("tm", None, None), P("tm", None))
    return jax.shard_map(body, mesh=mesh, in_specs=in_specs, out_specs=out_specs, check_vma=False)
```

```python
import functools

import jax
import jax.numpy as jnp
from jax import lax
from jax.experimental import pallas as pl
from jax.experimental.pallas import tpu as pltpu
from jax.sharding import PartitionSpec as P

SHELLS = 128
LANES = 128
CORES = 2
MESH = pl.DeviceIdType.MESH


def kernel(
    snaps, slabs, rows,
    vel_ref, ids_ref, order_ref,
    coh_ref, spec_ref,
    staged, ids, order, got, split, terms, lhs, hot, mine, packs, near, mid, far, total, ready,
    load_sem, stage_sem, send_sem, recv_sem, near_send, near_recv, far_send, far_recv,
):
    tm = lax.axis_index("tm")
    slab = lax.axis_index("slab")
    core = lax.rem(slab, CORES)
    place = lax.div(slab, CORES)
    places = slabs // CORES
    pairs = snaps * snaps
    half = 3 * snaps // CORES

    others = []
    for high in reversed(range(snaps // 2)):
        for low in (1, 0):
            other_high = lax.rem(lax.div(tm, 2) + high, snaps // 2)
            others.append(other_high * 2 + lax.rem(lax.rem(tm, 2) + low, 2))
    others = others[:-1]
    other_core = CORES - 1 - core
    near_peers = [(other, other_core, 1) for other in others]
    near_peers += [(other, core, 0) for other in others]
    near_peers += [(tm, other_core, 1)]
    far_peers = []
    for offset in range(1, places):
        away = lax.rem(place + offset, places)
        far_peers += [(away, other_core, 1), (away, core, 0)]
    far_peers += [(place, other_core, 1)]

    barrier = pltpu.get_barrier_semaphore()
    for away, to_core, _ in far_peers[:-1]:
        pl.semaphore_signal(
            barrier, inc=1, device_id=(tm, away * CORES + to_core), device_id_type=MESH
        )
    for other, to_core, _ in near_peers:
        pl.semaphore_signal(
            barrier, inc=1, device_id=(other, place * CORES + to_core), device_id_type=MESH
        )

    def share_of(snap):
        return pl.ds(pl.multiple_of(snap * 2 * rows, 2 * rows), 2 * rows)

    stages = []
    for n, other in enumerate(others):
        stage = pltpu.make_async_copy(
            vel_ref.at[:, share_of(other)], staged.at[n], stage_sem.at[n]
        )
        stage.start()
        stages.append(stage)
    load_own = pltpu.make_async_copy(vel_ref.at[:, share_of(tm)], got.at[tm], load_sem.at[0])
    load_own.start()
    load_ids = pltpu.make_async_copy(
        ids_ref.at[pl.ds(pl.multiple_of(tm * rows, rows), rows)], ids, load_sem.at[1]
    )
    load_ids.start()
    load_order = pltpu.make_async_copy(order_ref, order, load_sem.at[2])
    load_order.start()

    pl.semaphore_wait(barrier, len(near_peers) + len(far_peers) - 1)
    moves = []
    for n, other in enumerate(others):
        stages[n].wait()
        move = pltpu.make_async_remote_copy(
            src_ref=staged.at[n],
            dst_ref=got.at[tm],
            send_sem=send_sem.at[n],
            recv_sem=recv_sem.at[n],
            device_id=(other, slab),
            device_id_type=MESH,
        )
        move.start()
        moves.append(move)

    load_ids.wait()
    shell = lax.broadcasted_iota(jnp.int32, (SHELLS, LANES), 0)
    for j in range(rows):
        same = shell == jnp.broadcast_to(ids[j : j + 1, :], (SHELLS, LANES))
        hot[:, j * LANES : (j + 1) * LANES] = jnp.where(same, 1.0, 0.0).astype(jnp.bfloat16)

    load_order.wait()
    load_own.wait()
    for move in moves:
        move.wait()

    real, imag = {}, {}
    for t in range(snaps):
        for c in range(3):
            split[t * 3 + c] = got[t, c].astype(jnp.float32)
    for t in range(snaps):
        for c in range(3):
            real[t, c] = split[t * 3 + c, pl.ds(0, rows, stride=2), :]
            imag[t, c] = split[t * 3 + c, pl.ds(1, rows, stride=2), :]

    for t in range(snaps):
        for r in range(t, snaps):
            value = real[t, 0] * real[r, 0] + imag[t, 0] * imag[r, 0]
            for c in (1, 2):
                value = value + real[t, c] * real[r, c]
                value = value + imag[t, c] * imag[r, c]
            terms[(t * snaps + r) * rows : (t * snaps + r + 1) * rows] = value
            if r > t:
                value = imag[t, 0] * real[r, 0] - real[t, 0] * imag[r, 0]
                for c in (1, 2):
                    value = value + imag[t, c] * real[r, c]
                    value = value - real[t, c] * imag[r, c]
                terms[(r * snaps + t) * rows : (r * snaps + t + 1) * rows] = value
    for j in range(rows):
        block = terms[pl.ds(j, pairs, stride=rows), :]
        lhs[:, j * LANES : (j + 1) * LANES] = block.astype(jnp.bfloat16)
    mine[...] = lax.dot_general(
        lhs[...], hot[...], (((1,), (1,)), ((), ())), preferred_element_type=jnp.float32
    )

    mid_rows = snaps // 2
    for t in range(snaps):
        packs[t, 0, :snaps] = mine[t * snaps : (t + 1) * snaps, :]
        packs[t, 0, snaps:half] = mine[pl.ds(t, mid_rows, stride=snaps), :]
        packs[t, 1, :mid_rows] = mine[pl.ds(t + mid_rows * snaps, mid_rows, stride=snaps), :]
        packs[t, 1, mid_rows:half] = mine[pl.ds(0, snaps, stride=snaps + 1), :]

    copies = []
    for n, (other, to_core, _) in enumerate(near_peers):
        copy = pltpu.make_async_remote_copy(
            src_ref=packs.at[other, to_core],
            dst_ref=near.at[n],
            send_sem=near_send.at[n],
            recv_sem=near_recv.at[n],
            device_id=(other, place * CORES + to_core),
            device_id_type=MESH,
        )
        copy.start()
        copies.append(copy)
    value = packs[tm, core]
    for n in reversed(range(len(near_peers))):
        copies[n].wait()
        value = value + near[n]
    mid[...] = value

    copies = []
    for n, (away, to_core, _) in enumerate(far_peers):
        copy = pltpu.make_async_remote_copy(
            src_ref=mid,
            dst_ref=far.at[n],
            send_sem=far_send.at[n],
            recv_sem=far_recv.at[n],
            device_id=(tm, away * CORES + to_core),
            device_id_type=MESH,
        )
        copy.start()
        copies.append(copy)
    sums = [mid[...], None]
    for n in reversed(range(len(far_peers))):
        copies[n].wait()
        turn = far_peers[n][2]
        sums[turn] = far[n] if sums[turn] is None else sums[turn] + far[n]
    total[core] = sums[0]
    total[other_core] = sums[1]

    across = total[0, :snaps]
    own_spectrum = total[0, pl.ds(tm, 1), :]
    ready[:mid_rows] = total[0, snaps:half]
    ready[mid_rows:] = total[1, :mid_rows]
    down = ready[...]
    spectra = total[1, mid_rows:half]
    which = lax.broadcasted_iota(jnp.int32, (snaps, SHELLS), 0)
    down = jnp.where(which == tm, 0.0, down)
    ready[...] = (across * across + down * down) / (own_spectrum * spectra)
    for j in range(snaps):
        coh_ref[0, j : j + 1, :] = ready[pl.ds(order[j], 1), :]
    spec_ref[...] = own_spectrum


def body(velocity, shell_index, ref_order):
    snaps = lax.axis_size("tm")
    slabs = lax.axis_size("slab")
    modes = velocity.shape[3]
    blocks = modes // LANES
    rows = blocks // snaps
    pairs = snaps * snaps
    vel = velocity.reshape(3, 2, blocks, LANES).transpose(0, 2, 1, 3)
    vel = vel.reshape(3, 2 * blocks, LANES)
    ids = shell_index.reshape(blocks, LANES)
    near = snaps * CORES - 1
    far = slabs - 1
    half = 3 * snaps // CORES
    return pl.pallas_call(
        functools.partial(kernel, snaps, slabs, rows),
        out_shape=(
            pltpu.VMEM((1, snaps, SHELLS), jnp.float32),
            pltpu.VMEM((1, SHELLS), jnp.float32),
        ),
        in_specs=[
            pl.BlockSpec(memory_space=pl.ANY),
            pl.BlockSpec(memory_space=pl.ANY),
            pl.BlockSpec(memory_space=pl.ANY),
        ],
        out_specs=(
            pl.BlockSpec(memory_space=pltpu.VMEM),
            pl.BlockSpec(memory_space=pltpu.VMEM),
        ),
        scratch_shapes=[
            pltpu.VMEM((snaps - 1, 3, 2 * rows, LANES), jnp.bfloat16),
            pltpu.VMEM((rows, LANES), jnp.int32),
            pltpu.SMEM((snaps,), jnp.int32),
            pltpu.VMEM((snaps, 3, 2 * rows, LANES), jnp.bfloat16),
            pltpu.VMEM((snaps * 3, 2 * rows, LANES), jnp.float32),
            pltpu.VMEM((pairs * rows, LANES), jnp.float32),
            pltpu.VMEM((pairs, rows * LANES), jnp.bfloat16),
            pltpu.VMEM((SHELLS, rows * LANES), jnp.bfloat16),
            pltpu.VMEM((pairs, SHELLS), jnp.float32),
            pltpu.VMEM((snaps, CORES, half, SHELLS), jnp.float32),
            pltpu.VMEM((near, half, SHELLS), jnp.float32),
            pltpu.VMEM((half, SHELLS), jnp.float32),
            pltpu.VMEM((far, half, SHELLS), jnp.float32),
            pltpu.VMEM((CORES, half, SHELLS), jnp.float32),
            pltpu.VMEM((snaps, SHELLS), jnp.float32),
            pltpu.SemaphoreType.DMA((3,)),
            pltpu.SemaphoreType.DMA((snaps - 1,)),
            pltpu.SemaphoreType.DMA((snaps - 1,)),
            pltpu.SemaphoreType.DMA((snaps - 1,)),
            pltpu.SemaphoreType.DMA((near,)),
            pltpu.SemaphoreType.DMA((near,)),
            pltpu.SemaphoreType.DMA((far,)),
            pltpu.SemaphoreType.DMA((far,)),
        ],
        compiler_params=pltpu.CompilerParams(collective_id=0, has_side_effects=True),
    )(vel, ids, ref_order)


def solution(mesh):
    in_specs = (P("tm", None, None, "slab"), P("slab"), P())
    out_specs = (P("tm", None, None), P("tm", None))
    return jax.shard_map(body, mesh=mesh, in_specs=in_specs, out_specs=out_specs, check_vma=False)
```

```python
import functools

import jax
import jax.numpy as jnp
from jax import lax
from jax.experimental import pallas as pl
from jax.experimental.pallas import tpu as pltpu
from jax.sharding import PartitionSpec as P

SHELLS = 128
LANES = 128
CORES = 2
MESH = pl.DeviceIdType.MESH


def kernel(
    snaps, slabs, rows,
    vel_ref, ids_ref, order_ref,
    coh_ref, spec_ref,
    staged, ids, order, got, split, terms, lhs, hot, mine, packs, near, mid, far, total, ready,
    load_sem, stage_sem, send_sem, recv_sem, near_send, near_recv, far_send, far_recv,
):
    tm = lax.axis_index("tm")
    slab = lax.axis_index("slab")
    core = lax.rem(slab, CORES)
    place = lax.div(slab, CORES)
    places = slabs // CORES
    pairs = snaps * snaps
    half = 3 * snaps // CORES

    others = []
    for high in reversed(range(snaps // 2)):
        for low in (1, 0):
            other_high = lax.rem(lax.div(tm, 2) + high, snaps // 2)
            others.append(other_high * 2 + lax.rem(lax.rem(tm, 2) + low, 2))
    others = others[:-1]
    other_core = CORES - 1 - core
    near_peers = [(other, other_core, 1) for other in others]
    near_peers += [(other, core, 0) for other in others]
    near_peers += [(tm, other_core, 1)]
    far_peers = []
    for offset in range(1, places):
        away = lax.rem(place + offset, places)
        far_peers += [(away, other_core, 1), (away, core, 0)]
    far_peers += [(place, other_core, 1)]

    barrier = pltpu.get_barrier_semaphore()
    for away, to_core, _ in far_peers[:-1]:
        pl.semaphore_signal(
            barrier, inc=1, device_id=(tm, away * CORES + to_core), device_id_type=MESH
        )
    for other, to_core, _ in near_peers:
        pl.semaphore_signal(
            barrier, inc=1, device_id=(other, place * CORES + to_core), device_id_type=MESH
        )

    def share_of(snap):
        return pl.ds(pl.multiple_of(snap * 2 * rows, 2 * rows), 2 * rows)

    for n, other in enumerate(others):
        pltpu.make_async_copy(vel_ref.at[:, share_of(other)], staged.at[n], stage_sem).start()
    load_own = pltpu.make_async_copy(vel_ref.at[:, share_of(tm)], got.at[tm], load_sem.at[0])
    load_own.start()
    load_ids = pltpu.make_async_copy(
        ids_ref.at[pl.ds(pl.multiple_of(tm * rows, rows), rows)], ids, load_sem.at[1]
    )
    load_ids.start()
    load_order = pltpu.make_async_copy(order_ref, order, load_sem.at[2])
    load_order.start()

    pl.semaphore_wait(barrier, len(near_peers) + len(far_peers) - 1)
    pltpu.make_async_copy(staged, staged, stage_sem).wait()
    for n, other in enumerate(others):
        move = pltpu.make_async_remote_copy(
            src_ref=staged.at[n],
            dst_ref=got.at[tm],
            send_sem=send_sem,
            recv_sem=recv_sem,
            device_id=(other, slab),
            device_id_type=MESH,
        )
        move.start()

    load_ids.wait()
    shell = lax.broadcasted_iota(jnp.int32, (SHELLS, LANES), 0)
    for j in range(rows):
        same = shell == jnp.broadcast_to(ids[j : j + 1, :], (SHELLS, LANES))
        hot[:, j * LANES : (j + 1) * LANES] = jnp.where(same, 1.0, 0.0).astype(jnp.bfloat16)

    load_order.wait()
    load_own.wait()
    pltpu.make_async_copy(staged, staged, recv_sem).wait()

    real, imag = {}, {}
    for t in range(snaps):
        for c in range(3):
            split[t * 3 + c] = got[t, c].astype(jnp.float32)
    for t in range(snaps):
        for c in range(3):
            real[t, c] = split[t * 3 + c, pl.ds(0, rows, stride=2), :]
            imag[t, c] = split[t * 3 + c, pl.ds(1, rows, stride=2), :]

    for t in range(snaps):
        for r in range(t, snaps):
            value = real[t, 0] * real[r, 0] + imag[t, 0] * imag[r, 0]
            for c in (1, 2):
                value = value + real[t, c] * real[r, c]
                value = value + imag[t, c] * imag[r, c]
            terms[(t * snaps + r) * rows : (t * snaps + r + 1) * rows] = value
            if r > t:
                value = imag[t, 0] * real[r, 0] - real[t, 0] * imag[r, 0]
                for c in (1, 2):
                    value = value + imag[t, c] * real[r, c]
                    value = value - real[t, c] * imag[r, c]
                terms[(r * snaps + t) * rows : (r * snaps + t + 1) * rows] = value
    for j in range(rows):
        block = terms[pl.ds(j, pairs, stride=rows), :]
        lhs[:, j * LANES : (j + 1) * LANES] = block.astype(jnp.bfloat16)
    mine[...] = lax.dot_general(
        lhs[...], hot[...], (((1,), (1,)), ((), ())), preferred_element_type=jnp.float32
    )

    mid_rows = snaps // 2
    for t in range(snaps):
        packs[t, 0, :snaps] = mine[t * snaps : (t + 1) * snaps, :]
        packs[t, 0, snaps:half] = mine[pl.ds(t, mid_rows, stride=snaps), :]
        packs[t, 1, :mid_rows] = mine[pl.ds(t + mid_rows * snaps, mid_rows, stride=snaps), :]
        packs[t, 1, mid_rows:half] = mine[pl.ds(0, snaps, stride=snaps + 1), :]

    for n, (other, to_core, _) in enumerate(near_peers):
        copy = pltpu.make_async_remote_copy(
            src_ref=packs.at[other, to_core],
            dst_ref=near.at[n * half : (n + 1) * half],
            send_sem=near_send,
            recv_sem=near_recv,
            device_id=(other, place * CORES + to_core),
            device_id_type=MESH,
        )
        copy.start()
    value = packs[tm, core]
    pltpu.make_async_copy(near, near, near_recv).wait()
    for n in range(len(near_peers)):
        value = value + near[n * half : (n + 1) * half]
    mid[...] = value

    for n, (away, to_core, _) in enumerate(far_peers):
        copy = pltpu.make_async_remote_copy(
            src_ref=mid,
            dst_ref=far.at[n * half : (n + 1) * half],
            send_sem=far_send,
            recv_sem=far_recv,
            device_id=(tm, away * CORES + to_core),
            device_id_type=MESH,
        )
        copy.start()
    sums = [mid[...], None]
    pltpu.make_async_copy(far, far, far_recv).wait()
    for n in range(len(far_peers)):
        turn = far_peers[n][2]
        term = far[n * half : (n + 1) * half]
        sums[turn] = term if sums[turn] is None else sums[turn] + term
    total[core] = sums[0]
    total[other_core] = sums[1]

    across = total[0, :snaps]
    own_spectrum = total[0, pl.ds(tm, 1), :]
    ready[:mid_rows] = total[0, snaps:half]
    ready[mid_rows:] = total[1, :mid_rows]
    down = ready[...]
    spectra = total[1, mid_rows:half]
    which = lax.broadcasted_iota(jnp.int32, (snaps, SHELLS), 0)
    down = jnp.where(which == tm, 0.0, down)
    ready[...] = (across * across + down * down) / (own_spectrum * spectra)
    for j in range(snaps):
        coh_ref[0, j : j + 1, :] = ready[pl.ds(order[j], 1), :]
    spec_ref[...] = own_spectrum
    pltpu.make_async_copy(staged, staged, send_sem).wait()
    pltpu.make_async_copy(near, near, near_send).wait()
    pltpu.make_async_copy(far, far, far_send).wait()


def put(coh_ref, spec_ref, coh_out, spec_out, sems):
    copies = [
        pltpu.make_async_copy(coh_ref, coh_out, sems.at[0]),
        pltpu.make_async_copy(spec_ref, spec_out, sems.at[1]),
    ]
    for copy in copies:
        copy.start()
    for copy in copies:
        copy.wait()


def body(velocity, shell_index, ref_order):
    snaps = lax.axis_size("tm")
    slabs = lax.axis_size("slab")
    modes = velocity.shape[3]
    blocks = modes // LANES
    rows = blocks // snaps
    pairs = snaps * snaps
    vel = velocity.reshape(3, 2, blocks, LANES).transpose(0, 2, 1, 3)
    vel = vel.reshape(3, 2 * blocks, LANES)
    ids = shell_index.reshape(blocks, LANES)
    near = snaps * CORES - 1
    far = slabs - 1
    half = 3 * snaps // CORES
    coherence, spectrum = pl.pallas_call(
        functools.partial(kernel, snaps, slabs, rows),
        out_shape=(
            pltpu.VMEM((1, snaps, SHELLS), jnp.float32),
            pltpu.VMEM((1, SHELLS), jnp.float32),
        ),
        in_specs=[
            pl.BlockSpec(memory_space=pl.ANY),
            pl.BlockSpec(memory_space=pl.ANY),
            pl.BlockSpec(memory_space=pl.ANY),
        ],
        out_specs=(
            pl.BlockSpec(memory_space=pltpu.VMEM),
            pl.BlockSpec(memory_space=pltpu.VMEM),
        ),
        scratch_shapes=[
            pltpu.VMEM((snaps - 1, 3, 2 * rows, LANES), jnp.bfloat16),
            pltpu.VMEM((rows, LANES), jnp.int32),
            pltpu.SMEM((snaps,), jnp.int32),
            pltpu.VMEM((snaps, 3, 2 * rows, LANES), jnp.bfloat16),
            pltpu.VMEM((snaps * 3, 2 * rows, LANES), jnp.float32),
            pltpu.VMEM((pairs * rows, LANES), jnp.float32),
            pltpu.VMEM((pairs, rows * LANES), jnp.bfloat16),
            pltpu.VMEM((SHELLS, rows * LANES), jnp.bfloat16),
            pltpu.VMEM((pairs, SHELLS), jnp.float32),
            pltpu.VMEM((snaps, CORES, half, SHELLS), jnp.float32),
            pltpu.VMEM((near * half, SHELLS), jnp.float32),
            pltpu.VMEM((half, SHELLS), jnp.float32),
            pltpu.VMEM((far * half, SHELLS), jnp.float32),
            pltpu.VMEM((CORES, half, SHELLS), jnp.float32),
            pltpu.VMEM((snaps, SHELLS), jnp.float32),
            pltpu.SemaphoreType.DMA((3,)),
            pltpu.SemaphoreType.DMA,
            pltpu.SemaphoreType.DMA,
            pltpu.SemaphoreType.DMA,
            pltpu.SemaphoreType.DMA,
            pltpu.SemaphoreType.DMA,
            pltpu.SemaphoreType.DMA,
            pltpu.SemaphoreType.DMA,
        ],
        compiler_params=pltpu.CompilerParams(collective_id=0, has_side_effects=True),
    )(vel, ids, ref_order)
    coherence = pltpu.with_memory_space_constraint(coherence, pltpu.VMEM)
    spectrum = pltpu.with_memory_space_constraint(spectrum, pltpu.VMEM)
    return pl.pallas_call(
        put,
        out_shape=(
            jax.ShapeDtypeStruct((1, snaps, SHELLS), jnp.float32),
            jax.ShapeDtypeStruct((1, SHELLS), jnp.float32),
        ),
        in_specs=[pl.BlockSpec(memory_space=pltpu.VMEM)] * 2,
        out_specs=(pl.BlockSpec(memory_space=pl.ANY),) * 2,
        scratch_shapes=[pltpu.SemaphoreType.DMA((2,))],
    )(coherence, spectrum)


def solution(mesh):
    in_specs = (P("tm", None, None, "slab"), P("slab"), P())
    out_specs = (P("tm", None, None), P("tm", None))
    return jax.shard_map(body, mesh=mesh, in_specs=in_specs, out_specs=out_specs, check_vma=False)
```
